32 devices in a mesh: tile: 8 (over y, x, core), pos: 4 (over z).
Axes of the slice: x: 2, y: 2, z: 4, core: 2. Of those that a mesh axis runs over, the one named last changes fastest.
Arguments:
- object_tiles: float32 [8, 2, 512, 512], P('tile'), may hold values from -5 to 5
- probe: float32 [2, 256, 256], replicated, may hold values from -6 to 6
- patterns: bfloat16 [256, 256, 256], P(('tile', 'pos')), may hold values from 0 to 4
- corners: int32 [256, 2], P(('tile', 'pos')), may hold values from 0 to 511, as said below
- counts: int32 [32], P(('tile', 'pos')), may hold values from 1 to 7, as said below
Outputs:
- refined: float32 [8, 2, 512, 512], P('tile')
The draws below stay inside these ranges and needn't reach their ends.
Inputs may be any that keep to these rules, and one draw needn't show every extreme that they name: `corners`: tile t sits in grid cell (t + 8 + 8 // 2) mod 8 of a row-major grid of 8 tiles a row. A corner row is at most 256 for slots of tiles in the grid's last row, a corner column at most 256 for slots of tiles in the grid's last column, so every crop lies inside the object. The device at tile index t and the one at tile index t + 4 with the same pos index have counts that sum to exactly 8; some device has 7.
All inputs are finite; a program needn't handle non-finite values.
Results may differ from the reference program's by a relative error of at most 0.018.
Values may be sent and summed in bfloat16 or wider, within the bound.
No kernel may reach another device: no remote copies, remote signals or barrier semaphores. Data moves between devices by JAX's collectives and lax.ppermute only.
A program may use at most 64 MiB of HBM per device.

```python
import math
import jax
import jax.numpy as jnp
from jax import lax

W = 256
TILE = 512
TILE_COLS = 8
SLOTS = 8
ITERS = 2
TILES = 8
SHARERS = 4
TILE_ROWS = 1
POSITIONS = 256


def draw_corners(key, part):
    slot_ids = jnp.arange(POSITIONS, dtype=jnp.int32)
    tile_ids = slot_ids // (SLOTS * SHARERS)
    cell_ids = (tile_ids + TILE_COLS + TILE_COLS // 2) % TILES
    first_slot = slot_ids % SLOTS == 0
    last_row = cell_ids // TILE_COLS == TILE_ROWS - 1
    last_col = cell_ids % TILE_COLS == TILE_COLS - 1
    row_limit = jnp.where(last_row, TILE - W + 1, TILE).astype(jnp.int32)
    col_limit = jnp.where(last_col, TILE - W + 1, TILE).astype(jnp.int32)
    row_floor = jnp.where(first_slot & jnp.logical_not(last_row), TILE - W + 1, 0).astype(jnp.int32)
    col_floor = jnp.where(first_slot & jnp.logical_not(last_col), TILE - W + 1, 0).astype(jnp.int32)
    row_key = jax.random.fold_in(key, 11)
    col_key = jax.random.fold_in(key, 12)
    corner_rows = jax.random.randint(row_key, (POSITIONS,), row_floor, row_limit, dtype=jnp.int32)
    corner_cols = jax.random.randint(col_key, (POSITIONS,), col_floor, col_limit, dtype=jnp.int32)
    return jnp.stack([corner_rows, corner_cols], 1)


def draw_counts(key, part):
    lower_half = jax.random.randint(jax.random.fold_in(key, 21), (TILES // 2, SHARERS), 1, SLOTS, dtype=jnp.int32)
    lower_half = lower_half.at[0, 0].set(SLOTS - 1)
    upper_half = SLOTS - lower_half
    return jnp.concatenate([lower_half, upper_half], 0).reshape(TILES * SHARERS).astype(jnp.int32)


def steps_of(rng, dims, cuts, smallest, high):
    gain, own = 1.0, jax.random.fold_in(rng, 6)
    for position, blocks in cuts:
        draws = jnp.exp(jax.random.uniform(jax.random.fold_in(own, position), (blocks,), jnp.float32, smallest / len(cuts), high / len(cuts)))
        gain = gain * jnp.repeat(draws, dims[position] // blocks).reshape([-1 if axis == position else 1 for axis in range(len(dims))])
    return gain


def bell_draw(rng, shape, width, most, split=(), kind=jnp.bfloat16):
    level = steps_of(rng, shape, split, -0.22, 0.18) if split else 1.0
    entries = jax.random.normal(rng, shape, jnp.float32) * width * level
    return jnp.minimum(jnp.maximum(entries, -most), most).astype(kind)


def setup_inputs(seed: int = 0) -> dict:
    splits = jax.random.split(jax.random.key(seed), 6)
    return {
        "object_tiles": bell_draw(splits[0], (TILES, 2, TILE, TILE), 0.7, 5.0, ((0, 8),), jnp.float32),
        "probe": bell_draw(splits[1], (2, W, W), 1.0, 6.0, (), jnp.float32),
        "patterns": jnp.clip(4.0 * jax.random.uniform(splits[2], (POSITIONS, W, W), jnp.float32) ** steps_of(splits[2], (POSITIONS, W, W), ((0, 32),), -0.2, 0.2), 0.0, 4.0).astype(jnp.bfloat16),
        "corners": draw_corners(jax.random.fold_in(splits[5], 71), 0),
        "counts": draw_counts(jax.random.fold_in(splits[5], 71), 0),
    }


LEARNING_RATE = 0.03

def tables(extent):
    counter = jnp.arange(extent, dtype=jnp.int32)
    phases = counter[:, None] * counter[None, :] % extent
    angles = phases.astype(jnp.float32) * (2.0 * math.pi / extent)
    factor = 1.0 / math.sqrt(extent)
    cosine = jnp.cos(angles) * factor
    sine_neg = -jnp.sin(angles) * factor
    forward_right = jnp.concatenate([jnp.concatenate([cosine, sine_neg], 1), jnp.concatenate([-sine_neg, cosine], 1)], 0).astype(jnp.bfloat16)
    forward_left = jnp.concatenate([cosine, sine_neg], 0).astype(jnp.bfloat16)
    backward_right = jnp.concatenate([jnp.concatenate([cosine, -sine_neg], 1), jnp.concatenate([sine_neg, cosine], 1)], 0).astype(jnp.bfloat16)
    backward_left = jnp.concatenate([cosine, -sine_neg], 0).astype(jnp.bfloat16)
    return (forward_right, forward_left, backward_right, backward_left)

def transform(waves, right_table, left_table):
    number, extent = (waves.shape[0], waves.shape[1])
    halfway = jnp.dot(waves.reshape(number * extent, 2 * extent), right_table, preferred_element_type=jnp.float32)
    halfway = lax.optimization_barrier(halfway.reshape(number, extent, 2 * extent).astype(jnp.bfloat16))
    stacked = jnp.einsum('jk,skl->sjl', left_table.astype(jnp.float32), halfway.astype(jnp.float32))
    upper = stacked[:, :extent]
    lower = stacked[:, extent:]
    real_part = upper[:, :, :extent] - lower[:, :, extent:]
    imag_part = upper[:, :, extent:] + lower[:, :, :extent]
    return jnp.concatenate([real_part, imag_part], 2)

def wave_gradient(waves, measured, table_set):
    extent = waves.shape[1]
    spectrum = transform(waves, table_set[0], table_set[1])
    power = spectrum[:, :, :extent] ** 2 + spectrum[:, :, extent:] ** 2
    misfit = power - measured.astype(jnp.float32)
    pushed = (spectrum * jnp.concatenate([misfit, misfit], 2)).astype(jnp.bfloat16)
    return transform(pushed, table_set[2], table_set[3]).astype(jnp.bfloat16)

def exit_waves(probe, crops):
    real_part = probe[0] * crops[:, 0] - probe[1] * crops[:, 1]
    imag_part = probe[0] * crops[:, 1] + probe[1] * crops[:, 0]
    return jnp.concatenate([real_part, imag_part], 2).astype(jnp.bfloat16)

def crop_gradients(probe, wave_grads, alive_mask):
    extent = probe.shape[1]
    real_in = wave_grads[:, :, :extent].astype(jnp.float32)
    imag_in = wave_grads[:, :, extent:].astype(jnp.float32)
    real_part = probe[0] * real_in + probe[1] * imag_in
    imag_part = probe[0] * imag_in - probe[1] * real_in
    return jnp.stack([real_part, imag_part], 1) * alive_mask[:, None, None, None]

def reference(object_tiles, probe, patterns, corners, counts):
    table_set = tables(W)
    rotation = (TILE_COLS + TILE_COLS // 2) % TILES
    cell_tiles = jnp.roll(object_tiles, rotation, axis=0)
    full_object = cell_tiles.reshape(TILE_ROWS, TILE_COLS, 2, TILE, TILE).transpose(2, 0, 3, 1, 4)
    full_object = full_object.reshape(2, TILE_ROWS * TILE, TILE_COLS * TILE)
    slot_ids = jnp.arange(POSITIONS, dtype=jnp.int32)
    device_ids = slot_ids // SLOTS
    tile_ids = device_ids // SHARERS
    cell_ids = (tile_ids + rotation) % TILES
    anchor_rows = (cell_ids // TILE_COLS * TILE + corners[:, 0]).astype(jnp.int32)
    anchor_cols = (cell_ids % TILE_COLS * TILE + corners[:, 1]).astype(jnp.int32)
    live_flags = (slot_ids % SLOTS < counts[device_ids]).astype(jnp.float32)
    for repeat in range(ITERS):
        current = full_object

        def visit_slot(running, scan_item):
            row_at, col_at, measured, alive_flag = scan_item
            anchor = (jnp.zeros((), jnp.int32), row_at, col_at)
            window_crop = lax.dynamic_slice(current, anchor, (2, W, W))
            waves = exit_waves(probe, window_crop[None])
            wave_grads = wave_gradient(waves, measured[None], table_set)
            portion = crop_gradients(probe, wave_grads, alive_flag[None])[0]
            region = lax.dynamic_slice(running, anchor, (2, W, W))
            return (lax.dynamic_update_slice(running, region + portion, anchor), None)
        zeros_image = jnp.zeros(current.shape, jnp.float32)
        grad_image, _ = lax.scan(visit_slot, zeros_image, (anchor_rows, anchor_cols, patterns, live_flags))
        full_object = current - LEARNING_RATE * grad_image
    refined = full_object.reshape(2, TILE_ROWS, TILE, TILE_COLS, TILE).transpose(1, 3, 0, 2, 4)
    refined = refined.reshape(TILES, 2, TILE, TILE)
    return jnp.roll(refined, -rotation, axis=0)
```

```python
import functools
import math

import jax
import jax.numpy as jnp
import numpy as np
from jax import lax
from jax.experimental import pallas as pl
from jax.experimental.pallas import tpu as pltpu
from jax.sharding import PartitionSpec as P

TILE_COLS = 8
ITERS = 2
LEARNING_RATE = 0.03
LANES = 128
SUBLANES = 8
VMEM = pltpu.VMEM
SMEM = pltpu.SMEM


def tables(extent):
    counter = np.arange(extent)
    angles = (counter[:, None] * counter[None, :] % extent) * (2.0 * math.pi / extent)
    cosine = np.cos(angles) / math.sqrt(extent)
    sine_neg = -np.sin(angles) / math.sqrt(extent)
    cosine, sine_neg = (jnp.asarray(v, jnp.float32).astype(jnp.bfloat16) for v in (cosine, sine_neg))
    first = jnp.concatenate(
        [jnp.concatenate([cosine, sine_neg], 1), jnp.concatenate([-sine_neg, cosine], 1)], 0
    )
    second = jnp.concatenate(
        [jnp.concatenate([cosine, -sine_neg], 1), jnp.concatenate([sine_neg, cosine], 1)], 0
    )
    return first, second


def transform(side_by_side, right_table, left_table):
    extent = side_by_side.shape[0]
    halfway = jnp.dot(side_by_side, right_table, preferred_element_type=jnp.float32).astype(
        jnp.bfloat16
    )
    stacked = jnp.concatenate([halfway[:, :extent], halfway[:, extent:]], 0)
    return jnp.dot(left_table, stacked, preferred_element_type=jnp.float32)


def visit_slots(corners, counts, probe, patterns, first, second, extended, grad):
    extent = patterns.shape[1]
    rows_iota = lax.broadcasted_iota(jnp.int32, (SUBLANES, LANES), 0)
    lane_iota = lax.broadcasted_iota(jnp.int32, (extent, LANES), 1)

    def visit(slot, carry):
        row_at = corners[slot, 0]
        col_at = corners[slot, 1]
        row_base = pl.multiple_of(row_at // SUBLANES * SUBLANES, SUBLANES)
        col_base = pl.multiple_of(col_at // LANES * LANES, LANES)
        row_turn = row_at - row_base
        col_turn = col_at - col_base
        col_next = pl.multiple_of(col_base + LANES, LANES)
        col_wrap = pl.multiple_of(col_base + extent, LANES)
        row_wrap = pl.multiple_of(row_base + extent, SUBLANES)
        wrapped_lane = lane_iota < col_turn
        wrapped_row = rows_iota < row_turn

        def column(plane, col):
            body = extended[plane, pl.ds(row_base, extent), pl.ds(col, LANES)]
            tail = extended[plane, pl.ds(row_wrap, SUBLANES), pl.ds(col, LANES)]
            top = jnp.where(wrapped_row, tail, body[:SUBLANES])
            return jnp.concatenate([top, body[SUBLANES:]], 0)

        def window(plane):
            left = jnp.where(wrapped_lane, column(plane, col_wrap), column(plane, col_base))
            return jnp.concatenate([left, column(plane, col_next)], 1)

        def turned(plane):
            return pltpu.roll(pltpu.roll(probe[plane], row_turn, 0), col_turn, 1)

        probe_re = turned(0)
        probe_im = turned(1)
        crop_re = window(0)
        crop_im = window(1)
        wave = jnp.concatenate(
            [
                (probe_re * crop_re - probe_im * crop_im).astype(jnp.bfloat16),
                (probe_re * crop_im + probe_im * crop_re).astype(jnp.bfloat16),
            ],
            1,
        )
        spectrum = transform(wave, first[...], second[...])
        real = spectrum[:extent]
        imag = spectrum[extent:]
        misfit = real * real + imag * imag - patterns[slot].astype(jnp.float32)
        pushed = jnp.concatenate(
            [(misfit * real).astype(jnp.bfloat16), (misfit * imag).astype(jnp.bfloat16)], 1
        )
        wave_grad = transform(pushed, second[...], first[...]).astype(jnp.bfloat16)
        grad_re = wave_grad[:extent].astype(jnp.float32)
        grad_im = wave_grad[extent:].astype(jnp.float32)

        def add_column(plane, col, value):
            body = pl.ds(pl.multiple_of(row_base + SUBLANES, SUBLANES), extent - SUBLANES)
            grad[plane, body, pl.ds(col, LANES)] += value[SUBLANES:]
            top = value[:SUBLANES]
            grad[plane, pl.ds(row_base, SUBLANES), pl.ds(col, LANES)] += jnp.where(
                wrapped_row, 0.0, top
            )
            grad[plane, pl.ds(row_wrap, SUBLANES), pl.ds(col, LANES)] += jnp.where(
                wrapped_row, top, 0.0
            )

        def add_window(plane, value):
            left = value[:, :LANES]
            add_column(plane, col_base, jnp.where(wrapped_lane, 0.0, left))
            add_column(plane, col_next, value[:, LANES:])
            add_column(plane, col_wrap, jnp.where(wrapped_lane, left, 0.0))

        add_window(0, probe_re * grad_re + probe_im * grad_im)
        add_window(1, probe_re * grad_im - probe_im * grad_re)
        return carry

    lax.fori_loop(0, counts[0], visit, 0)


def row_kernel(
    with_update,
    corners,
    counts,
    plane_index,
    tile,
    margin,
    probe,
    patterns,
    first,
    second,
    *rest,
):
    if with_update:
        left_own, left_other, right_own, right_other, margin_own, margin_other, *rest = rest
    (
        left_send,
        left_keep,
        margin_send,
        margin_cross,
        right_send,
        right_keep,
        *rest,
    ) = rest
    if with_update:
        tile_out, *rest = rest
    extended, grad = rest
    extent = probe.shape[1]
    edge = tile.shape[1]
    own = plane_index[0]
    other = 1 - own
    if with_update:
        for plane, pieces in (
            (own, (left_own, right_own, margin_own)),
            (other, (left_other, right_other, margin_other)),
        ):
            for block, piece in enumerate(pieces):
                step = LEARNING_RATE * piece[...].astype(jnp.float32)
                cols = slice(block * extent, (block + 1) * extent)
                if block * extent < edge:
                    value = tile[plane, :, cols] - step
                    tile_out[plane, :, cols] = value
                else:
                    value = margin[plane].astype(jnp.float32) - step
                extended[plane, :edge, cols] = value
    else:
        for plane in (0, 1):
            extended[plane, :edge, :edge] = tile[plane]
            extended[plane, :edge, edge:] = margin[plane].astype(jnp.float32)
    grad[...] = jnp.zeros_like(grad)
    visit_slots(corners, counts, probe, patterns, first, second, extended, grad)
    left = slice(0, extent)
    right = slice(extent, edge)
    beyond = slice(edge, edge + extent)
    left_send[...] = grad[other, :edge, left].astype(jnp.bfloat16)
    left_keep[...] = grad[own, :edge, left]
    margin_send[...] = grad[own, :edge, beyond].astype(jnp.bfloat16)
    margin_cross[...] = grad[other, :edge, beyond].astype(jnp.bfloat16)
    right_send[...] = grad[other, :edge, right].astype(jnp.bfloat16)
    right_keep[...] = grad[own, :edge, right]


def row_step(corners, counts, plane_index, tile, margin, probe, patterns, table_set, pieces):
    extent = probe.shape[1]
    edge = tile.shape[1]
    slots = patterns.shape[0]
    half = jax.ShapeDtypeStruct((edge, extent), jnp.bfloat16)
    wide = jax.ShapeDtypeStruct((edge, extent), jnp.float32)
    outs = [half, wide, half, half, half, wide]
    if pieces:
        outs.append(jax.ShapeDtypeStruct(tile.shape, jnp.float32))
    whole = pl.BlockSpec(memory_space=VMEM)
    scalar = pl.BlockSpec(memory_space=SMEM)
    return pl.pallas_call(
        functools.partial(row_kernel, bool(pieces)),
        out_shape=outs,
        in_specs=[scalar] * 3 + [whole] * (6 + len(pieces)),
        out_specs=[whole] * len(outs),
        scratch_shapes=[
            pltpu.VMEM((2, edge + SUBLANES, edge + extent), jnp.float32),
            pltpu.VMEM((2, edge + SUBLANES, edge + extent), jnp.float32),
        ],
        cost_estimate=pl.CostEstimate(
            flops=slots * 32 * extent**3, bytes_accessed=8 * edge * edge, transcendentals=0
        ),
        compiler_params=pltpu.CompilerParams(vmem_limit_bytes=40 << 20),
    )(corners, counts, plane_index, tile, margin, probe, patterns, *table_set, *pieces)


def finish_kernel(plane_index, tile, left_own, left_other, right_own, right_other, out):
    own = plane_index[0]
    extent = left_own.shape[1]
    for plane, pieces in ((own, (left_own, right_own)), (1 - own, (left_other, right_other))):
        for block, piece in enumerate(pieces):
            cols = slice(block * extent, (block + 1) * extent)
            step = LEARNING_RATE * piece[...].astype(jnp.float32)
            out[plane, :, cols] = tile[plane, :, cols] - step


def finish(plane_index, tile, pieces):
    whole = pl.BlockSpec(memory_space=VMEM)
    return pl.pallas_call(
        finish_kernel,
        out_shape=jax.ShapeDtypeStruct(tile.shape, jnp.float32),
        in_specs=[pl.BlockSpec(memory_space=SMEM)] + [whole] * 5,
        out_specs=whole,
    )(plane_index, tile, *pieces)


def tile_pairs(count, row_shift, col_shift, grid_rows):
    turn = TILE_COLS + TILE_COLS // 2
    pairs = []
    for source in range(count):
        cell = (source + turn) % count
        row = cell // TILE_COLS + row_shift
        col = cell % TILE_COLS + col_shift
        if 0 <= row < grid_rows and 0 <= col < TILE_COLS:
            pairs.append((source, (row * TILE_COLS + col - turn) % count))
    return pairs


def move(value, pairs, sharers, mask):
    both = [
        (source * sharers + pos, target * sharers + (pos ^ mask))
        for source, target in pairs
        for pos in range(sharers)
    ]
    return lax.ppermute(value, ("tile", "pos"), both)


def row_shards(object_tile, probe, patterns, corners, counts, table_set):
    tile_count = lax.axis_size("tile")
    sharers = lax.axis_size("pos")
    extent = probe.shape[1]
    here = [(tile, tile) for tile in range(tile_count)]
    onward = tile_pairs(tile_count, 0, 1, 1)
    back = tile_pairs(tile_count, 0, -1, 1)
    plane_index = (lax.axis_index("pos") % 2).reshape(1).astype(jnp.int32)
    margin = move(object_tile[:, :, :extent].astype(jnp.bfloat16), back, sharers, 0)
    total = lambda *values: sum(value.astype(jnp.float32) for value in values).astype(jnp.bfloat16)
    pieces = ()
    for repeat in range(ITERS):
        left_send, left_keep, margin_send, margin_cross, right_send, right_keep, *rest = row_step(
            corners, counts, plane_index, object_tile, margin, probe, patterns, table_set, pieces
        )
        if rest:
            object_tile = rest[0]
        left_got = move(left_send, here, sharers, 1)
        cross_got = move(margin_cross, onward, sharers, 1)
        margin_got = move(margin_send, onward, sharers, 0)
        right_got = move(right_send, here, sharers, 1)
        left_pair = total(left_keep, left_got, margin_got, cross_got)
        left_far = move(left_pair, here, sharers, 2)
        right_pair = total(right_keep, right_got)
        right_far = move(right_pair, here, sharers, 2)
        left_own = total(left_pair, left_far)
        left_other = move(left_own, here, sharers, 1)
        last = repeat == ITERS - 1
        if not last:
            margin_own = move(left_own, back, sharers, 0)
            margin_other = move(left_own, back, sharers, 1)
        right_own = total(right_pair, right_far)
        right_other = move(right_own, here, sharers, 1)
        pieces = (left_own, left_other, right_own, right_other)
        if not last:
            pieces += (margin_own, margin_other)
    return finish(plane_index, object_tile, pieces)


def plain_kernel(corners, counts, extended, probe, patterns, first, second, out, *scratch):
    padded, grad = scratch
    rows = extended.shape[1]
    padded[:, :rows, :] = extended[...]
    grad[...] = jnp.zeros_like(grad)
    visit_slots(corners, counts, probe, patterns, first, second, padded, grad)
    out[...] = grad[:, :rows, :]


def plain_step(corners, counts, extended, probe, patterns, table_set):
    extent = probe.shape[1]
    rows, cols = extended.shape[1:]
    whole = pl.BlockSpec(memory_space=VMEM)
    return pl.pallas_call(
        plain_kernel,
        out_shape=jax.ShapeDtypeStruct(extended.shape, jnp.float32),
        in_specs=[pl.BlockSpec(memory_space=SMEM)] * 2 + [whole] * 5,
        out_specs=whole,
        scratch_shapes=[
            pltpu.VMEM((2, rows + SUBLANES, cols), jnp.float32),
            pltpu.VMEM((2, rows + SUBLANES, cols), jnp.float32),
        ],
        compiler_params=pltpu.CompilerParams(vmem_limit_bytes=48 << 20),
    )(corners, counts, extended, probe, patterns, *table_set)


def grid_shards(object_tile, probe, patterns, corners, counts, table_set):
    tile_count = lax.axis_size("tile")
    sharers = lax.axis_size("pos")
    grid_rows = tile_count // TILE_COLS
    extent = probe.shape[1]
    edge = object_tile.shape[1]

    def shift(value, rows, cols):
        pairs = tile_pairs(tile_count, rows, cols, grid_rows)
        return move(value.astype(jnp.bfloat16), pairs, sharers, 0).astype(jnp.float32)

    for repeat in range(ITERS):
        upper = jnp.concatenate([object_tile, shift(object_tile[:, :, :extent], 0, -1)], 2)
        lower = jnp.concatenate(
            [
                shift(object_tile[:, :extent, :], -1, 0),
                shift(object_tile[:, :extent, :extent], -1, -1),
            ],
            2,
        )
        extended = jnp.concatenate([upper, lower], 1)
        grad = plain_step(corners, counts, extended, probe, patterns, table_set)
        interior = grad[:, :edge, :edge]
        interior = interior.at[:, :, :extent].add(shift(grad[:, :edge, edge:], 0, 1))
        interior = interior.at[:, :extent, :].add(shift(grad[:, edge:, :edge], 1, 0))
        interior = interior.at[:, :extent, :extent].add(shift(grad[:, edge:, edge:], 1, 1))
        object_tile = object_tile - LEARNING_RATE * lax.psum(
            interior.astype(jnp.bfloat16), "pos"
        ).astype(jnp.float32)
    return object_tile


def shards(object_tiles, probe, patterns, corners, counts):
    table_set = tables(probe.shape[1])
    one_row = lax.axis_size("tile") == TILE_COLS
    paired = lax.axis_size("pos") == 4 and object_tiles.shape[2] == 2 * probe.shape[1]
    run = row_shards if one_row and paired else grid_shards
    return run(object_tiles[0], probe, patterns, corners, counts, table_set)[None]


def solution(mesh):
    return jax.shard_map(
        shards,
        mesh=mesh,
        in_specs=(
            P("tile", None, None, None),
            P(),
            P(("tile", "pos"), None, None),
            P(("tile", "pos"), None),
            P(("tile", "pos")),
        ),
        out_specs=P("tile", None, None, None),
        check_vma=False,
    )
```

```python
import functools
import math

import jax
import jax.numpy as jnp
import numpy as np
from jax import lax
from jax.experimental import pallas as pl
from jax.experimental.pallas import tpu as pltpu
from jax.sharding import PartitionSpec as P

TILE_COLS = 8
ITERS = 2
LEARNING_RATE = 0.03
LANES = 128
SUBLANES = 8
LIMIT = 24 << 20
VMEM = pltpu.VMEM
SMEM = pltpu.SMEM
HBM = pltpu.MemorySpace.HBM


def tables(extent):
    counter = np.arange(extent)
    angles = (counter[:, None] * counter[None, :] % extent) * (2.0 * math.pi / extent)
    cosine = np.cos(angles) / math.sqrt(extent)
    sine_neg = -np.sin(angles) / math.sqrt(extent)
    cosine, sine_neg = (jnp.asarray(v, jnp.float32).astype(jnp.bfloat16) for v in (cosine, sine_neg))
    first = jnp.concatenate(
        [jnp.concatenate([cosine, sine_neg], 1), jnp.concatenate([-sine_neg, cosine], 1)], 0
    )
    second = jnp.concatenate(
        [jnp.concatenate([cosine, -sine_neg], 1), jnp.concatenate([sine_neg, cosine], 1)], 0
    )
    return first, second


def transform(side_by_side, right_table, left_table):
    extent = side_by_side.shape[0]
    halfway = jnp.dot(side_by_side, right_table, preferred_element_type=jnp.float32).astype(
        jnp.bfloat16
    )
    stacked = jnp.concatenate([halfway[:, :extent], halfway[:, extent:]], 0)
    return jnp.dot(left_table, stacked, preferred_element_type=jnp.float32)


def visit_slots(chosen, corners, counts, probe, patterns, first, second, extended, grad):
    extent = patterns.shape[1]
    rows_iota = lax.broadcasted_iota(jnp.int32, (SUBLANES, LANES), 0)
    lane_iota = lax.broadcasted_iota(jnp.int32, (extent, LANES), 1)

    def visit(slot):
        row_at = corners[slot, 0]
        col_at = corners[slot, 1]
        row_base = pl.multiple_of(row_at // SUBLANES * SUBLANES, SUBLANES)
        col_base = pl.multiple_of(col_at // LANES * LANES, LANES)
        row_turn = row_at - row_base
        col_turn = col_at - col_base
        col_next = pl.multiple_of(col_base + LANES, LANES)
        col_wrap = pl.multiple_of(col_base + extent, LANES)
        row_wrap = pl.multiple_of(row_base + extent, SUBLANES)
        wrapped_lane = lane_iota < col_turn
        wrapped_row = rows_iota < row_turn

        def column(plane, col):
            body = extended[plane, pl.ds(row_base, extent), pl.ds(col, LANES)]
            tail = extended[plane, pl.ds(row_wrap, SUBLANES), pl.ds(col, LANES)]
            top = jnp.where(wrapped_row, tail, body[:SUBLANES])
            return jnp.concatenate([top, body[SUBLANES:]], 0)

        def window(plane):
            left = jnp.where(wrapped_lane, column(plane, col_wrap), column(plane, col_base))
            return jnp.concatenate([left, column(plane, col_next)], 1)

        def turned(plane):
            return pltpu.roll(pltpu.roll(probe[plane], row_turn, 0), col_turn, 1)

        probe_re = turned(0)
        probe_im = turned(1)
        crop_re = window(0)
        crop_im = window(1)
        wave = jnp.concatenate(
            [
                (probe_re * crop_re - probe_im * crop_im).astype(jnp.bfloat16),
                (probe_re * crop_im + probe_im * crop_re).astype(jnp.bfloat16),
            ],
            1,
        )
        spectrum = transform(wave, first[...], second[...])
        real = spectrum[:extent]
        imag = spectrum[extent:]
        misfit = real * real + imag * imag - patterns[slot].astype(jnp.float32)
        pushed = jnp.concatenate(
            [(misfit * real).astype(jnp.bfloat16), (misfit * imag).astype(jnp.bfloat16)], 1
        )
        wave_grad = transform(pushed, second[...], first[...]).astype(jnp.bfloat16)
        grad_re = wave_grad[:extent].astype(jnp.float32)
        grad_im = wave_grad[extent:].astype(jnp.float32)

        def add_column(plane, col, value):
            body = pl.ds(pl.multiple_of(row_base + SUBLANES, SUBLANES), extent - SUBLANES)
            grad[plane, body, pl.ds(col, LANES)] += value[SUBLANES:]
            top = value[:SUBLANES]
            grad[plane, pl.ds(row_base, SUBLANES), pl.ds(col, LANES)] += jnp.where(
                wrapped_row, 0.0, top
            )
            grad[plane, pl.ds(row_wrap, SUBLANES), pl.ds(col, LANES)] += jnp.where(
                wrapped_row, top, 0.0
            )

        def add_window(plane, value):
            left = value[:, :LANES]
            add_column(plane, col_base, jnp.where(wrapped_lane, 0.0, left))
            add_column(plane, col_next, value[:, LANES:])
            add_column(plane, col_wrap, jnp.where(wrapped_lane, left, 0.0))

        add_window(0, probe_re * grad_re + probe_im * grad_im)
        add_window(1, probe_re * grad_im - probe_im * grad_re)

    def step(slot, carry):
        pl.when(chosen(corners[slot, 1]))(functools.partial(visit, slot))
        return carry

    lax.fori_loop(0, counts[0], step, 0)


def block_of(index, extent):
    return (
        slice(index % 2 * extent, (index % 2 + 1) * extent),
        slice(index // 2 * extent, (index // 2 + 1) * extent),
    )


def take_step(extended, pieces, own, first_index):
    extent = pieces[0].shape[1]
    count = len(pieces) // 2
    for index, piece in enumerate(pieces):
        plane = own if index < count else 1 - own
        rows, cols = block_of(first_index + index % count, extent)
        extended[plane, rows, cols] -= LEARNING_RATE * piece[...].astype(jnp.float32)


def load_kernel(edge, corners, counts, tile, *rest):
    loads, (extended, grad, *held), sems = rest[:4], rest[4:10], rest[10]
    copies = [
        pltpu.make_async_copy(source, target, sems.at[index])
        for index, (source, target) in enumerate(
            zip((tile, *loads), (extended.at[:, :edge, :edge], *held))
        )
    ]
    for copy in copies:
        copy.start()
    grad[...] = jnp.zeros_like(grad)
    for copy in copies:
        copy.wait()
    extent = held[0].shape[1]
    visit_slots(lambda col: col + extent <= edge, corners, counts, *held, extended, grad)


def inner_kernel(edge, corners, counts, plane_index, *rest):
    held, pieces, (extended, grad) = rest[:4], rest[6:14], rest[14:]
    grad[...] = jnp.zeros_like(grad)
    take_step(extended, pieces, plane_index[0], 0)
    extent = held[0].shape[1]
    visit_slots(lambda col: col + extent <= edge, corners, counts, *held, extended, grad)


def outer_kernel(edge, corners, counts, plane_index, *rest):
    held, rest = rest[:4], rest[6:]
    margins, (extended, grad, margin_send, *halves) = rest[:-11], rest[-11:]
    extent = held[0].shape[1]
    own = plane_index[0]
    other = 1 - own
    beyond = slice(edge, edge + extent)
    if len(margins) == 1:
        for plane in (0, 1):
            extended[plane, :edge, beyond] = margins[0][plane].astype(jnp.float32)
    else:
        take_step(extended, margins, own, 4)
    visit_slots(lambda col: col + extent > edge, corners, counts, *held, extended, grad)
    margin_send[0] = grad[own, :edge, beyond].astype(jnp.bfloat16)
    margin_send[1] = grad[other, :edge, beyond].astype(jnp.bfloat16)
    for index, half in enumerate(halves):
        rows, cols = block_of(index // 4 * 2 + index % 2, extent)
        plane = (own, other)[index % 4 // 2]
        half[...] = grad[plane, rows, cols].astype(half.dtype)


WHOLE = pl.BlockSpec(memory_space=VMEM)
SCALAR = pl.BlockSpec(memory_space=SMEM)


def slot_cost(extent, slots):
    return pl.CostEstimate(
        flops=slots * 16 * extent**3, bytes_accessed=64 * extent * extent, transcendentals=0
    )


def load_step(corners, counts, tile, probe, patterns, table_set):
    extent = probe.shape[1]
    edge = tile.shape[1]
    loads = (probe, patterns, *table_set)
    image = jax.ShapeDtypeStruct((2, edge + SUBLANES, edge + extent), jnp.float32)
    extended, grad, *held = pl.pallas_call(
        functools.partial(load_kernel, edge),
        out_shape=[image, image] + [jax.ShapeDtypeStruct(v.shape, v.dtype) for v in loads],
        in_specs=[SCALAR] * 2 + [pl.BlockSpec(memory_space=HBM)] * 5,
        out_specs=[WHOLE] * 6,
        scratch_shapes=[pltpu.SemaphoreType.DMA((5,))],
        cost_estimate=slot_cost(extent, patterns.shape[0]),
        compiler_params=pltpu.CompilerParams(vmem_limit_bytes=LIMIT),
    )(corners, counts, *(pltpu.with_memory_space_constraint(v, HBM) for v in (tile, *loads)))
    return extended, grad, held


def inner_step(corners, counts, plane_index, held, extended, grad, edge, pieces):
    return pl.pallas_call(
        functools.partial(inner_kernel, edge),
        out_shape=[jax.ShapeDtypeStruct(v.shape, v.dtype) for v in (extended, grad)],
        in_specs=[SCALAR] * 3 + [WHOLE] * (6 + len(pieces)),
        out_specs=[WHOLE] * 2,
        input_output_aliases={7: 0, 8: 1},
        cost_estimate=slot_cost(held[0].shape[1], held[1].shape[0]),
        compiler_params=pltpu.CompilerParams(vmem_limit_bytes=LIMIT),
    )(corners, counts, plane_index, *held, extended, grad, *pieces)


def outer_step(corners, counts, plane_index, held, extended, grad, edge, margins):
    extent = held[0].shape[1]
    half = jax.ShapeDtypeStruct((extent, extent), jnp.bfloat16)
    wide = jax.ShapeDtypeStruct((extent, extent), jnp.float32)
    outs = [jax.ShapeDtypeStruct(v.shape, v.dtype) for v in (extended, grad)]
    outs.append(jax.ShapeDtypeStruct((2, edge, extent), jnp.bfloat16))
    outs += [wide] * 6 + [half] * 2
    extended, grad, margin_send, *halves = pl.pallas_call(
        functools.partial(outer_kernel, edge),
        out_shape=outs,
        in_specs=[SCALAR] * 3 + [WHOLE] * (6 + len(margins)),
        out_specs=[WHOLE] * len(outs),
        input_output_aliases={7: 0, 8: 1},
        cost_estimate=slot_cost(extent, held[1].shape[0]),
        compiler_params=pltpu.CompilerParams(vmem_limit_bytes=LIMIT),
    )(corners, counts, plane_index, *held, extended, grad, *margins)
    return extended, grad, margin_send, halves


def finish_kernel(block, plane_index, extended, own_top, own_low, other_top, other_low, *rest):
    out = rest[-1]
    own = plane_index[0]
    extent = own_top.shape[0]
    for plane, pieces in ((own, (own_top, own_low)), (1 - own, (other_top, other_low))):
        for half, piece in enumerate(pieces):
            rows, cols = block_of(2 * block + half, extent)
            step = LEARNING_RATE * piece[...].astype(jnp.float32)
            out[plane, rows] = extended[plane, rows, cols] - step


def finish(plane_index, extended, edge, pieces, block, partial):
    extent = pieces[0].shape[1]
    column = pl.BlockSpec((2, edge, extent), lambda step: (0, 0, block))
    earlier = [] if partial is None else [partial]
    return pl.pallas_call(
        functools.partial(finish_kernel, block),
        grid=(1,),
        out_shape=jax.ShapeDtypeStruct((2, edge, edge), jnp.float32),
        in_specs=[SCALAR] + [WHOLE] * 5 + [pl.BlockSpec(memory_space=pl.ANY)] * len(earlier),
        out_specs=column,
        input_output_aliases={6: 0} if earlier else {},
        cost_estimate=pl.CostEstimate(
            flops=4 * edge * edge, bytes_accessed=12 * edge * edge, transcendentals=0
        ),
        compiler_params=pltpu.CompilerParams(vmem_limit_bytes=LIMIT),
    )(plane_index, extended, *pieces, *earlier)


def tile_pairs(count, row_shift, col_shift, grid_rows):
    turn = TILE_COLS + TILE_COLS // 2
    pairs = []
    for source in range(count):
        cell = (source + turn) % count
        row = cell // TILE_COLS + row_shift
        col = cell % TILE_COLS + col_shift
        if 0 <= row < grid_rows and 0 <= col < TILE_COLS:
            pairs.append((source, (row * TILE_COLS + col - turn) % count))
    return pairs


def move(value, pairs, sharers, mask):
    both = [
        (source * sharers + pos, target * sharers + (pos ^ mask))
        for source, target in pairs
        for pos in range(sharers)
    ]
    return lax.ppermute(value, ("tile", "pos"), both)


def total_wide(*values):
    return sum(value.astype(jnp.float32) for value in values)


def total(*values):
    return total_wide(*values).astype(jnp.bfloat16)


def share(keep, send, here, sharers):
    got = [move(value, here, sharers, 1) for value in send]
    pair = [total(*values) for values in zip(keep, got)]
    far = [move(value, here, sharers, 3) for value in pair]
    own = [total(*values) for values in zip(pair, far)]
    other = [move(value, here, sharers, 1) for value in own]
    return own, other


def row_shards(object_tile, probe, patterns, corners, counts, table_set):
    tile_count = lax.axis_size("tile")
    sharers = lax.axis_size("pos")
    extent = probe.shape[1]
    here = [(tile, tile) for tile in range(tile_count)]
    onward = tile_pairs(tile_count, 0, 1, 1)
    back = tile_pairs(tile_count, 0, -1, 1)
    pos = lax.axis_index("pos")
    plane_index = ((pos ^ (pos // 2)) % 2).reshape(1).astype(jnp.int32)
    margin = move(object_tile[:, :, :extent].astype(jnp.bfloat16), back, sharers, 0)
    edge = object_tile.shape[1]
    extended, grad, held = load_step(corners, counts, object_tile, probe, patterns, table_set)
    margins = [margin]
    for repeat in range(ITERS):
        extended, grad, margin_send, halves = outer_step(
            corners, counts, plane_index, held, extended, grad, edge, margins
        )
        left_keep, left_send, right_keep, right_send = (halves[i : i + 2] for i in range(0, 8, 2))
        margin_got = move(margin_send, onward, sharers, 0)
        right_own, right_other = share(right_keep, right_send, here, sharers)
        own_got, other_got = (
            [margin_got[plane, rows : rows + extent] for rows in (0, extent)] for plane in (0, 1)
        )
        left_keep = [total_wide(*pair) for pair in zip(left_keep, own_got)]
        left_send = [total(*pair) for pair in zip(left_send, other_got)]
        left_own, left_other = share(left_keep, left_send, here, sharers)
        if repeat < ITERS - 1:
            margins = [move(value, back, sharers, 0) for value in (*left_own, *left_other)]
            pieces = (*left_own, *right_own, *left_other, *right_other)
            extended, grad = inner_step(
                corners, counts, plane_index, held, extended, grad, edge, pieces
            )
    refined = finish(plane_index, extended, edge, (*right_own, *right_other), 1, None)
    return finish(plane_index, extended, edge, (*left_own, *left_other), 0, refined)


def plain_kernel(corners, counts, extended, probe, patterns, first, second, out, *scratch):
    padded, grad = scratch
    rows = extended.shape[1]
    padded[:, :rows, :] = extended[...]
    grad[...] = jnp.zeros_like(grad)
    every = lambda col_at: col_at >= 0
    visit_slots(every, corners, counts, probe, patterns, first, second, padded, grad)
    out[...] = grad[:, :rows, :]


def plain_step(corners, counts, extended, probe, patterns, table_set):
    extent = probe.shape[1]
    rows, cols = extended.shape[1:]
    whole = pl.BlockSpec(memory_space=VMEM)
    return pl.pallas_call(
        plain_kernel,
        out_shape=jax.ShapeDtypeStruct(extended.shape, jnp.float32),
        in_specs=[pl.BlockSpec(memory_space=SMEM)] * 2 + [whole] * 5,
        out_specs=whole,
        scratch_shapes=[
            pltpu.VMEM((2, rows + SUBLANES, cols), jnp.float32),
            pltpu.VMEM((2, rows + SUBLANES, cols), jnp.float32),
        ],
        compiler_params=pltpu.CompilerParams(vmem_limit_bytes=48 << 20),
    )(corners, counts, extended, probe, patterns, *table_set)


def grid_shards(object_tile, probe, patterns, corners, counts, table_set):
    tile_count = lax.axis_size("tile")
    sharers = lax.axis_size("pos")
    grid_rows = tile_count // TILE_COLS
    extent = probe.shape[1]
    edge = object_tile.shape[1]

    def shift(value, rows, cols):
        pairs = tile_pairs(tile_count, rows, cols, grid_rows)
        return move(value.astype(jnp.bfloat16), pairs, sharers, 0).astype(jnp.float32)

    for repeat in range(ITERS):
        upper = jnp.concatenate([object_tile, shift(object_tile[:, :, :extent], 0, -1)], 2)
        lower = jnp.concatenate(
            [
                shift(object_tile[:, :extent, :], -1, 0),
                shift(object_tile[:, :extent, :extent], -1, -1),
            ],
            2,
        )
        extended = jnp.concatenate([upper, lower], 1)
        grad = plain_step(corners, counts, extended, probe, patterns, table_set)
        interior = grad[:, :edge, :edge]
        interior = interior.at[:, :, :extent].add(shift(grad[:, :edge, edge:], 0, 1))
        interior = interior.at[:, :extent, :].add(shift(grad[:, edge:, :edge], 1, 0))
        interior = interior.at[:, :extent, :extent].add(shift(grad[:, edge:, edge:], 1, 1))
        object_tile = object_tile - LEARNING_RATE * lax.psum(
            interior.astype(jnp.bfloat16), "pos"
        ).astype(jnp.float32)
    return object_tile


def shards(object_tiles, probe, patterns, corners, counts):
    table_set = tables(probe.shape[1])
    one_row = lax.axis_size("tile") == TILE_COLS
    paired = lax.axis_size("pos") == 4 and object_tiles.shape[2] == 2 * probe.shape[1]
    run = row_shards if one_row and paired else grid_shards
    return run(object_tiles[0], probe, patterns, corners, counts, table_set)[None]


def solution(mesh):
    return jax.shard_map(
        shards,
        mesh=mesh,
        in_specs=(
            P("tile", None, None, None),
            P(),
            P(("tile", "pos"), None, None),
            P(("tile", "pos"), None),
            P(("tile", "pos")),
        ),
        out_specs=P("tile", None, None, None),
        check_vma=False,
    )
```

```python
import functools
import math

import jax
import jax.numpy as jnp
import numpy as np
from jax import lax
from jax.experimental import pallas as pl
from jax.experimental.pallas import tpu as pltpu
from jax.sharding import PartitionSpec as P

TILE_COLS = 8
ITERS = 2
LEARNING_RATE = 0.03
LANES = 128
SUBLANES = 8
LIMIT = 24 << 20
VMEM = pltpu.VMEM
SMEM = pltpu.SMEM
HBM = pltpu.MemorySpace.HBM


def tables(extent):
    counter = np.arange(extent)
    angles = (counter[:, None] * counter[None, :] % extent) * (2.0 * math.pi / extent)
    cosine = np.cos(angles) / math.sqrt(extent)
    sine_neg = -np.sin(angles) / math.sqrt(extent)
    cosine, sine_neg = (jnp.asarray(v, jnp.float32).astype(jnp.bfloat16) for v in (cosine, sine_neg))
    first = jnp.concatenate(
        [jnp.concatenate([cosine, sine_neg], 1), jnp.concatenate([-sine_neg, cosine], 1)], 0
    )
    second = jnp.concatenate(
        [jnp.concatenate([cosine, -sine_neg], 1), jnp.concatenate([sine_neg, cosine], 1)], 0
    )
    return first, second


def side_to_stack(planes):
    extent = planes.shape[0]
    return jnp.concatenate([planes[:, :extent], planes[:, extent:]], 0)


def visit_slots(
    chosen, corners, counts, probe, patterns, first, second, extended, grad, work
):
    order, wave_ref, turned_ref = work
    extent = patterns.shape[1]
    rows_iota = lax.broadcasted_iota(jnp.int32, (SUBLANES, LANES), 0)
    lane_iota = lax.broadcasted_iota(jnp.int32, (extent, LANES), 1)

    def place(slot):
        row_at = corners[slot, 0]
        col_at = corners[slot, 1]
        row_base = pl.multiple_of(row_at // SUBLANES * SUBLANES, SUBLANES)
        col_base = pl.multiple_of(col_at // LANES * LANES, LANES)
        col_next = pl.multiple_of(col_base + LANES, LANES)
        col_wrap = pl.multiple_of(col_base + extent, LANES)
        row_wrap = pl.multiple_of(row_base + extent, SUBLANES)
        return row_at - row_base, col_at - col_base, row_base, row_wrap, col_base, col_next, col_wrap

    def prepare(slot, side):
        row_turn, col_turn, row_base, row_wrap, col_base, col_next, col_wrap = place(slot)
        wrapped_lane = lane_iota < col_turn
        wrapped_row = rows_iota < row_turn

        def column(plane, col):
            body = extended[plane, pl.ds(row_base, extent), pl.ds(col, LANES)]
            tail = extended[plane, pl.ds(row_wrap, SUBLANES), pl.ds(col, LANES)]
            top = jnp.where(wrapped_row, tail, body[:SUBLANES])
            return jnp.concatenate([top, body[SUBLANES:]], 0)

        def window(plane):
            left = jnp.where(wrapped_lane, column(plane, col_wrap), column(plane, col_base))
            return jnp.concatenate([left, column(plane, col_next)], 1)

        def turned(plane):
            return pltpu.roll(pltpu.roll(probe[plane], row_turn, 0), col_turn, 1)

        probe_re = turned(0)
        probe_im = turned(1)
        turned_ref[side, 0] = probe_re
        turned_ref[side, 1] = probe_im
        crop_re = window(0)
        crop_im = window(1)
        wave_ref[:, :extent] = (probe_re * crop_re - probe_im * crop_im).astype(jnp.bfloat16)
        wave_ref[:, extent:] = (probe_re * crop_im + probe_im * crop_re).astype(jnp.bfloat16)

    def visit(index, carry):
        slot = order[index]
        side = index % 2
        halfway = jnp.dot(wave_ref[...], first[...], preferred_element_type=jnp.float32)
        halfway = side_to_stack(halfway.astype(jnp.bfloat16))
        prepare(order[jnp.minimum(index + 1, live - 1)], 1 - side)
        spectrum = jnp.dot(second[...], halfway, preferred_element_type=jnp.float32)
        real = spectrum[:extent]
        imag = spectrum[extent:]
        misfit = real * real + imag * imag - patterns[slot].astype(jnp.float32)
        pushed = jnp.concatenate(
            [(misfit * real).astype(jnp.bfloat16), (misfit * imag).astype(jnp.bfloat16)], 1
        )
        backhalf = jnp.dot(pushed, second[...], preferred_element_type=jnp.float32)
        backhalf = side_to_stack(backhalf.astype(jnp.bfloat16))
        wave_grad = jnp.dot(first[...], backhalf, preferred_element_type=jnp.float32)
        wave_grad = wave_grad.astype(jnp.bfloat16)
        grad_re = wave_grad[:extent].astype(jnp.float32)
        grad_im = wave_grad[extent:].astype(jnp.float32)
        row_turn, col_turn, row_base, row_wrap, col_base, col_next, col_wrap = place(slot)
        wrapped_lane = lane_iota < col_turn
        wrapped_row = rows_iota < row_turn
        probe_re = turned_ref[side, 0]
        probe_im = turned_ref[side, 1]

        def add_column(plane, col, value):
            body = pl.ds(pl.multiple_of(row_base + SUBLANES, SUBLANES), extent - SUBLANES)
            grad[plane, body, pl.ds(col, LANES)] += value[SUBLANES:]
            top = value[:SUBLANES]
            grad[plane, pl.ds(row_base, SUBLANES), pl.ds(col, LANES)] += jnp.where(
                wrapped_row, 0.0, top
            )
            grad[plane, pl.ds(row_wrap, SUBLANES), pl.ds(col, LANES)] += jnp.where(
                wrapped_row, top, 0.0
            )

        def add_window(plane, value):
            left = value[:, :LANES]
            add_column(plane, col_base, jnp.where(wrapped_lane, 0.0, left))
            add_column(plane, col_next, value[:, LANES:])
            add_column(plane, col_wrap, jnp.where(wrapped_lane, left, 0.0))

        add_window(0, probe_re * grad_re + probe_im * grad_im)
        add_window(1, probe_re * grad_im - probe_im * grad_re)

        return carry

    def choose(slot, found):
        order[found] = slot
        return found + chosen(corners[slot, 1]).astype(jnp.int32)

    live = lax.fori_loop(0, counts[0], choose, 0)
    pl.when(live > 0)(lambda: prepare(order[0], 0))
    lax.fori_loop(0, live, visit, 0)


def work_space(extent, slots):
    return [
        pltpu.SMEM((slots + 1,), jnp.int32),
        pltpu.VMEM((extent, 2 * extent), jnp.bfloat16),
        pltpu.VMEM((2, 2, extent, extent), jnp.float32),
    ]


def block_of(index, extent):
    return (
        slice(index % 2 * extent, (index % 2 + 1) * extent),
        slice(index // 2 * extent, (index // 2 + 1) * extent),
    )


def take_step(extended, pieces, own, first_block):
    row, index = 0, 0
    edge = pieces[0].shape[1] * 2
    blocks = sum(piece.shape[0] for piece in pieces) // edge // 2
    for piece in pieces:
        rows, extent = piece.shape
        plane = own if index < blocks else 1 - own
        start = (first_block + index % blocks) * extent
        cols = slice(start, start + extent)
        extended[plane, row : row + rows, cols] -= LEARNING_RATE * piece[...].astype(jnp.float32)
        row += rows
        if row == edge:
            row, index = 0, index + 1


def load_kernel(edge, corners, counts, tile, *rest):
    loads, (extended, grad, *held), (sems, *work) = rest[:4], rest[4:10], rest[10:]
    copies = [
        pltpu.make_async_copy(source, target, sems.at[index])
        for index, (source, target) in enumerate(
            zip((tile, *loads), (extended.at[:, :edge, :edge], *held))
        )
    ]
    for copy in copies:
        copy.start()
    grad[...] = jnp.zeros_like(grad)
    for copy in copies:
        copy.wait()
    extent = held[0].shape[1]
    visit_slots(lambda col: col + extent <= edge, corners, counts, *held, extended, grad, work)


def inner_kernel(edge, corners, counts, plane_index, *rest):
    rest, work = rest[:-3], rest[-3:]
    held, pieces, (extended, grad) = rest[:4], rest[6:14], rest[14:]
    grad[...] = jnp.zeros_like(grad)
    take_step(extended, pieces, plane_index[0], 0)
    extent = held[0].shape[1]
    visit_slots(lambda col: col + extent <= edge, corners, counts, *held, extended, grad, work)


def outer_kernel(edge, corners, counts, plane_index, *rest):
    rest, work = rest[:-3], rest[-3:]
    held, rest = rest[:4], rest[6:]
    margins, (extended, grad, margin_send, *halves) = rest[:-11], rest[-11:]
    extent = held[0].shape[1]
    own = plane_index[0]
    other = 1 - own
    beyond = slice(edge, edge + extent)
    if len(margins) == 1:
        for plane in (0, 1):
            extended[plane, :edge, beyond] = margins[0][plane].astype(jnp.float32)
    else:
        take_step(extended, margins, own, edge // extent)
    visit_slots(lambda col: col + extent > edge, corners, counts, *held, extended, grad, work)
    margin_send[0] = grad[own, :edge, beyond].astype(jnp.bfloat16)
    margin_send[1] = grad[other, :edge, beyond].astype(jnp.bfloat16)
    for index, half in enumerate(halves):
        rows, cols = block_of(index // 4 * 2 + index % 2, extent)
        plane = (own, other)[index % 4 // 2]
        half[...] = grad[plane, rows, cols].astype(half.dtype)


WHOLE = pl.BlockSpec(memory_space=VMEM)
SCALAR = pl.BlockSpec(memory_space=SMEM)


def slot_cost(extent, slots):
    return pl.CostEstimate(
        flops=slots * 16 * extent**3, bytes_accessed=64 * extent * extent, transcendentals=0
    )


def load_step(corners, counts, tile, probe, patterns, table_set):
    extent = probe.shape[1]
    edge = tile.shape[1]
    loads = (probe, patterns, *table_set)
    image = jax.ShapeDtypeStruct((2, edge + SUBLANES, edge + extent), jnp.float32)
    extended, grad, *held = pl.pallas_call(
        functools.partial(load_kernel, edge),
        out_shape=[image, image] + [jax.ShapeDtypeStruct(v.shape, v.dtype) for v in loads],
        in_specs=[SCALAR] * 2 + [pl.BlockSpec(memory_space=HBM)] * 5,
        out_specs=[WHOLE] * 6,
        scratch_shapes=[pltpu.SemaphoreType.DMA((5,)), *work_space(extent, patterns.shape[0])],
        cost_estimate=slot_cost(extent, patterns.shape[0]),
        compiler_params=pltpu.CompilerParams(vmem_limit_bytes=LIMIT),
    )(corners, counts, *(pltpu.with_memory_space_constraint(v, HBM) for v in (tile, *loads)))
    return extended, grad, held


def inner_step(corners, counts, plane_index, held, extended, grad, edge, pieces):
    return pl.pallas_call(
        functools.partial(inner_kernel, edge),
        out_shape=[jax.ShapeDtypeStruct(v.shape, v.dtype) for v in (extended, grad)],
        in_specs=[SCALAR] * 3 + [WHOLE] * (6 + len(pieces)),
        out_specs=[WHOLE] * 2,
        scratch_shapes=work_space(held[0].shape[1], held[1].shape[0]),
        input_output_aliases={7: 0, 8: 1},
        cost_estimate=slot_cost(held[0].shape[1], held[1].shape[0]),
        compiler_params=pltpu.CompilerParams(vmem_limit_bytes=LIMIT),
    )(corners, counts, plane_index, *held, extended, grad, *pieces)


def outer_step(corners, counts, plane_index, held, extended, grad, edge, margins):
    extent = held[0].shape[1]
    half = jax.ShapeDtypeStruct((extent, extent), jnp.bfloat16)
    wide = jax.ShapeDtypeStruct((extent, extent), jnp.float32)
    outs = [jax.ShapeDtypeStruct(v.shape, v.dtype) for v in (extended, grad)]
    outs.append(jax.ShapeDtypeStruct((2, edge, extent), jnp.bfloat16))
    outs += [wide] * 6 + [half] * 2
    extended, grad, margin_send, *halves = pl.pallas_call(
        functools.partial(outer_kernel, edge),
        out_shape=outs,
        in_specs=[SCALAR] * 3 + [WHOLE] * (6 + len(margins)),
        out_specs=[WHOLE] * len(outs),
        scratch_shapes=work_space(held[0].shape[1], held[1].shape[0]),
        input_output_aliases={7: 0, 8: 1},
        cost_estimate=slot_cost(extent, held[1].shape[0]),
        compiler_params=pltpu.CompilerParams(vmem_limit_bytes=LIMIT),
    )(corners, counts, plane_index, *held, extended, grad, *margins)
    return extended, grad, margin_send, halves


def finish_kernel(block, plane_index, extended, own_top, own_low, other_top, other_low, *rest):
    out = rest[-1]
    own = plane_index[0]
    extent = own_top.shape[0]
    for plane, pieces in ((own, (own_top, own_low)), (1 - own, (other_top, other_low))):
        for half, piece in enumerate(pieces):
            rows, cols = block_of(2 * block + half, extent)
            step = LEARNING_RATE * piece[...].astype(jnp.float32)
            out[plane, rows] = extended[plane, rows, cols] - step


def finish(plane_index, extended, edge, pieces, block, partial):
    extent = pieces[0].shape[1]
    column = pl.BlockSpec((2, edge, extent), lambda step: (0, 0, block))
    earlier = [] if partial is None else [partial]
    return pl.pallas_call(
        functools.partial(finish_kernel, block),
        grid=(1,),
        out_shape=jax.ShapeDtypeStruct((2, edge, edge), jnp.float32),
        in_specs=[SCALAR] + [WHOLE] * 5 + [pl.BlockSpec(memory_space=pl.ANY)] * len(earlier),
        out_specs=column,
        input_output_aliases={6: 0} if earlier else {},
        cost_estimate=pl.CostEstimate(
            flops=4 * edge * edge, bytes_accessed=12 * edge * edge, transcendentals=0
        ),
        compiler_params=pltpu.CompilerParams(vmem_limit_bytes=LIMIT),
    )(plane_index, extended, *pieces, *earlier)


def tile_pairs(count, row_shift, col_shift, grid_rows):
    turn = TILE_COLS + TILE_COLS // 2
    pairs = []
    for source in range(count):
        cell = (source + turn) % count
        row = cell // TILE_COLS + row_shift
        col = cell % TILE_COLS + col_shift
        if 0 <= row < grid_rows and 0 <= col < TILE_COLS:
            pairs.append((source, (row * TILE_COLS + col - turn) % count))
    return pairs


def move(value, pairs, sharers, mask):
    both = [
        (source * sharers + pos, target * sharers + (pos ^ mask))
        for source, target in pairs
        for pos in range(sharers)
    ]
    return lax.ppermute(value, ("tile", "pos"), both)


def total_wide(*values):
    return sum(value.astype(jnp.float32) for value in values)


def total(*values):
    return total_wide(*values).astype(jnp.bfloat16)


def share(keep, send, here, sharers):
    got = [move(value, here, sharers, 1) for value in send]
    pair = [total(*values) for values in zip(keep, got)]
    far = [move(value, here, sharers, 3) for value in pair]
    own = [total(*values) for values in zip(pair, far)]
    other = [move(value, here, sharers, 1) for value in own]
    return own, other


def row_shards(object_tile, probe, patterns, corners, counts, table_set):
    tile_count = lax.axis_size("tile")
    sharers = lax.axis_size("pos")
    extent = probe.shape[1]
    here = [(tile, tile) for tile in range(tile_count)]
    onward = tile_pairs(tile_count, 0, 1, 1)
    back = tile_pairs(tile_count, 0, -1, 1)
    pos = lax.axis_index("pos")
    plane_index = ((pos ^ (pos // 2)) % 2).reshape(1).astype(jnp.int32)
    margin = move(object_tile[:, :, :extent].astype(jnp.bfloat16), back, sharers, 0)
    edge = object_tile.shape[1]
    extended, grad, held = load_step(corners, counts, object_tile, probe, patterns, table_set)
    margins = [margin]
    for repeat in range(ITERS):
        extended, grad, margin_send, halves = outer_step(
            corners, counts, plane_index, held, extended, grad, edge, margins
        )
        left_keep, left_send, right_keep, right_send = (halves[i : i + 2] for i in range(0, 8, 2))
        margin_got = move(margin_send, onward, sharers, 0)
        right_own, right_other = share(right_keep, right_send, here, sharers)
        own_got, other_got = (
            [margin_got[plane, rows : rows + extent] for rows in (0, extent)] for plane in (0, 1)
        )
        left_keep = [total_wide(*pair) for pair in zip(left_keep, own_got)]
        left_send = [total(*pair) for pair in zip(left_send, other_got)]
        left_own, left_other = share(left_keep, left_send, here, sharers)
        if repeat < ITERS - 1:
            margins = [
                move(jnp.concatenate(value, 0), back, sharers, 0)
                for value in (left_own, left_other)
            ]
            pieces = (*left_own, *right_own, *left_other, *right_other)
            extended, grad = inner_step(
                corners, counts, plane_index, held, extended, grad, edge, pieces
            )
    refined = finish(plane_index, extended, edge, (*right_own, *right_other), 1, None)
    return finish(plane_index, extended, edge, (*left_own, *left_other), 0, refined)


def plain_kernel(corners, counts, extended, probe, patterns, first, second, out, *scratch):
    padded, grad, *work = scratch
    rows = extended.shape[1]
    padded[:, :rows, :] = extended[...]
    grad[...] = jnp.zeros_like(grad)
    every = lambda col_at: col_at >= 0
    visit_slots(every, corners, counts, probe, patterns, first, second, padded, grad, work)
    out[...] = grad[:, :rows, :]


def plain_step(corners, counts, extended, probe, patterns, table_set):
    extent = probe.shape[1]
    rows, cols = extended.shape[1:]
    whole = pl.BlockSpec(memory_space=VMEM)
    return pl.pallas_call(
        plain_kernel,
        out_shape=jax.ShapeDtypeStruct(extended.shape, jnp.float32),
        in_specs=[pl.BlockSpec(memory_space=SMEM)] * 2 + [whole] * 5,
        out_specs=whole,
        scratch_shapes=[
            pltpu.VMEM((2, rows + SUBLANES, cols), jnp.float32),
            pltpu.VMEM((2, rows + SUBLANES, cols), jnp.float32),
            *work_space(extent, patterns.shape[0]),
        ],
        compiler_params=pltpu.CompilerParams(vmem_limit_bytes=48 << 20),
    )(corners, counts, extended, probe, patterns, *table_set)


def grid_shards(object_tile, probe, patterns, corners, counts, table_set):
    tile_count = lax.axis_size("tile")
    sharers = lax.axis_size("pos")
    grid_rows = tile_count // TILE_COLS
    extent = probe.shape[1]
    edge = object_tile.shape[1]

    def shift(value, rows, cols):
        pairs = tile_pairs(tile_count, rows, cols, grid_rows)
        return move(value.astype(jnp.bfloat16), pairs, sharers, 0).astype(jnp.float32)

    for repeat in range(ITERS):
        upper = jnp.concatenate([object_tile, shift(object_tile[:, :, :extent], 0, -1)], 2)
        lower = jnp.concatenate(
            [
                shift(object_tile[:, :extent, :], -1, 0),
                shift(object_tile[:, :extent, :extent], -1, -1),
            ],
            2,
        )
        extended = jnp.concatenate([upper, lower], 1)
        grad = plain_step(corners, counts, extended, probe, patterns, table_set)
        interior = grad[:, :edge, :edge]
        interior = interior.at[:, :, :extent].add(shift(grad[:, :edge, edge:], 0, 1))
        interior = interior.at[:, :extent, :].add(shift(grad[:, edge:, :edge], 1, 0))
        interior = interior.at[:, :extent, :extent].add(shift(grad[:, edge:, edge:], 1, 1))
        object_tile = object_tile - LEARNING_RATE * lax.psum(
            interior.astype(jnp.bfloat16), "pos"
        ).astype(jnp.float32)
    return object_tile


def shards(object_tiles, probe, patterns, corners, counts):
    table_set = tables(probe.shape[1])
    one_row = lax.axis_size("tile") == TILE_COLS
    paired = lax.axis_size("pos") == 4 and object_tiles.shape[2] == 2 * probe.shape[1]
    run = row_shards if one_row and paired else grid_shards
    return run(object_tiles[0], probe, patterns, corners, counts, table_set)[None]


def solution(mesh):
    return jax.shard_map(
        shards,
        mesh=mesh,
        in_specs=(
            P("tile", None, None, None),
            P(),
            P(("tile", "pos"), None, None),
            P(("tile", "pos"), None),
            P(("tile", "pos")),
        ),
        out_specs=P("tile", None, None, None),
        check_vma=False,
    )
```

```python
import functools
import math

import jax
import jax.numpy as jnp
import numpy as np
from jax import lax
from jax.experimental import pallas as pl
from jax.experimental.pallas import tpu as pltpu
from jax.sharding import PartitionSpec as P

TILE_COLS = 8
ITERS = 2
LEARNING_RATE = 0.03
LANES = 128
SUBLANES = 8
LIMIT = 24 << 20
VMEM = pltpu.VMEM
SMEM = pltpu.SMEM
HBM = pltpu.MemorySpace.HBM


def tables(extent):
    counter = np.arange(extent)
    angles = (counter[:, None] * counter[None, :] % extent) * (2.0 * math.pi / extent)
    cosine = np.cos(angles) / math.sqrt(extent)
    sine_neg = -np.sin(angles) / math.sqrt(extent)
    cosine, sine_neg = (jnp.asarray(v, jnp.float32).astype(jnp.bfloat16) for v in (cosine, sine_neg))
    first = jnp.concatenate(
        [jnp.concatenate([cosine, sine_neg], 1), jnp.concatenate([-sine_neg, cosine], 1)], 0
    )
    second = jnp.concatenate(
        [jnp.concatenate([cosine, -sine_neg], 1), jnp.concatenate([sine_neg, cosine], 1)], 0
    )
    return first, second


def side_to_stack(planes):
    extent = planes.shape[0]
    return jnp.concatenate([planes[:, :extent], planes[:, extent:]], 0)


def visit_slots(
    chosen, corners, counts, probe, patterns, first, second, extended, grad, work
):
    order, wave_ref, turned_ref = work
    extent = patterns.shape[1]
    rows_iota = lax.broadcasted_iota(jnp.int32, (SUBLANES, LANES), 0)
    lane_iota = lax.broadcasted_iota(jnp.int32, (extent, LANES), 1)

    def place(slot):
        row_at = corners[0, slot]
        col_at = corners[1, slot]
        row_base = pl.multiple_of(row_at // SUBLANES * SUBLANES, SUBLANES)
        col_base = pl.multiple_of(col_at // LANES * LANES, LANES)
        col_next = pl.multiple_of(col_base + LANES, LANES)
        col_wrap = pl.multiple_of(col_base + extent, LANES)
        row_wrap = pl.multiple_of(row_base + extent, SUBLANES)
        return row_at - row_base, col_at - col_base, row_base, row_wrap, col_base, col_next, col_wrap

    def prepare(slot, side):
        row_turn, col_turn, row_base, row_wrap, col_base, col_next, col_wrap = place(slot)
        wrapped_lane = lane_iota < col_turn
        wrapped_row = rows_iota < row_turn

        def column(plane, col):
            body = extended[plane, pl.ds(row_base, extent), pl.ds(col, LANES)]
            tail = extended[plane, pl.ds(row_wrap, SUBLANES), pl.ds(col, LANES)]
            top = jnp.where(wrapped_row, tail, body[:SUBLANES])
            return jnp.concatenate([top, body[SUBLANES:]], 0)

        def window(plane):
            left = jnp.where(wrapped_lane, column(plane, col_wrap), column(plane, col_base))
            return jnp.concatenate([left, column(plane, col_next)], 1)

        def turned(plane):
            return pltpu.roll(pltpu.roll(probe[plane], row_turn, 0), col_turn, 1)

        probe_re = turned(0)
        probe_im = turned(1)
        turned_ref[side, 0] = probe_re
        turned_ref[side, 1] = probe_im
        crop_re = window(0)
        crop_im = window(1)
        wave_ref[:, :extent] = (probe_re * crop_re - probe_im * crop_im).astype(jnp.bfloat16)
        wave_ref[:, extent:] = (probe_re * crop_im + probe_im * crop_re).astype(jnp.bfloat16)

    def visit(index, carry):
        slot = order[index]
        side = index % 2
        halfway = jnp.dot(wave_ref[...], first[...], preferred_element_type=jnp.float32)
        halfway = side_to_stack(halfway.astype(jnp.bfloat16))
        prepare(order[jnp.minimum(index + 1, live - 1)], 1 - side)
        spectrum = jnp.dot(second[...], halfway, preferred_element_type=jnp.float32)
        real = spectrum[:extent]
        imag = spectrum[extent:]
        misfit = real * real + imag * imag - patterns[slot].astype(jnp.float32)
        pushed = jnp.concatenate(
            [(misfit * real).astype(jnp.bfloat16), (misfit * imag).astype(jnp.bfloat16)], 1
        )
        backhalf = jnp.dot(pushed, second[...], preferred_element_type=jnp.float32)
        backhalf = side_to_stack(backhalf.astype(jnp.bfloat16))
        wave_grad = jnp.dot(first[...], backhalf, preferred_element_type=jnp.float32)
        wave_grad = wave_grad.astype(jnp.bfloat16)
        grad_re = wave_grad[:extent].astype(jnp.float32)
        grad_im = wave_grad[extent:].astype(jnp.float32)
        row_turn, col_turn, row_base, row_wrap, col_base, col_next, col_wrap = place(slot)
        wrapped_lane = lane_iota < col_turn
        wrapped_row = rows_iota < row_turn
        probe_re = turned_ref[side, 0]
        probe_im = turned_ref[side, 1]

        def add_column(plane, col, value):
            body = pl.ds(pl.multiple_of(row_base + SUBLANES, SUBLANES), extent - SUBLANES)
            grad[plane, body, pl.ds(col, LANES)] += value[SUBLANES:]
            top = value[:SUBLANES]
            grad[plane, pl.ds(row_base, SUBLANES), pl.ds(col, LANES)] += jnp.where(
                wrapped_row, 0.0, top
            )
            grad[plane, pl.ds(row_wrap, SUBLANES), pl.ds(col, LANES)] += jnp.where(
                wrapped_row, top, 0.0
            )

        def add_window(plane, value):
            left = value[:, :LANES]
            add_column(plane, col_base, jnp.where(wrapped_lane, 0.0, left))
            add_column(plane, col_next, value[:, LANES:])
            add_column(plane, col_wrap, jnp.where(wrapped_lane, left, 0.0))

        add_window(0, probe_re * grad_re + probe_im * grad_im)
        add_window(1, probe_re * grad_im - probe_im * grad_re)

        return carry

    def choose(slot, found):
        order[found] = slot
        return found + chosen(corners[1, slot]).astype(jnp.int32)

    live = lax.fori_loop(0, counts[0], choose, 0)
    pl.when(live > 0)(lambda: prepare(order[0], 0))
    lax.fori_loop(0, live, visit, 0)


def work_space(extent, slots):
    return [
        pltpu.SMEM((slots + 1,), jnp.int32),
        pltpu.VMEM((extent, 2 * extent), jnp.bfloat16),
        pltpu.VMEM((2, 2, extent, extent), jnp.float32),
    ]


def block_of(index, extent):
    return (
        slice(index % 2 * extent, (index % 2 + 1) * extent),
        slice(index // 2 * extent, (index // 2 + 1) * extent),
    )


def take_step(extended, pieces, own, first_block):
    row, index = 0, 0
    edge = pieces[0].shape[1] * 2
    blocks = sum(piece.shape[0] for piece in pieces) // edge // 2
    for piece in pieces:
        rows, extent = piece.shape
        plane = own if index < blocks else 1 - own
        start = (first_block + index % blocks) * extent
        cols = slice(start, start + extent)
        extended[plane, row : row + rows, cols] -= LEARNING_RATE * piece[...].astype(jnp.float32)
        row += rows
        if row == edge:
            row, index = 0, index + 1


def load_kernel(edge, corners, counts, tile, *rest):
    loads, (extended, grad, *held), (sems, *work) = rest[:4], rest[4:10], rest[10:]
    copies = [
        pltpu.make_async_copy(source, target, sems.at[index])
        for index, (source, target) in enumerate(
            zip((tile, *loads), (extended.at[:, :edge, :edge], *held))
        )
    ]
    for copy in copies:
        copy.start()
    grad[...] = jnp.zeros_like(grad)
    for copy in copies:
        copy.wait()
    extent = held[0].shape[1]
    visit_slots(lambda col: col + extent <= edge, corners, counts, *held, extended, grad, work)


def inner_kernel(edge, corners, counts, plane_index, *rest):
    rest, work = rest[:-3], rest[-3:]
    held, pieces, (extended, grad) = rest[:4], rest[6:14], rest[14:]
    grad[...] = jnp.zeros_like(grad)
    take_step(extended, pieces, plane_index[0], 0)
    extent = held[0].shape[1]
    visit_slots(lambda col: col + extent <= edge, corners, counts, *held, extended, grad, work)


def outer_kernel(edge, corners, counts, plane_index, *rest):
    rest, work = rest[:-3], rest[-3:]
    held, rest = rest[:4], rest[6:]
    margins, (extended, grad, margin_other, margin_own, *halves) = rest[:-12], rest[-12:]
    extent = held[0].shape[1]
    own = plane_index[0]
    other = 1 - own
    beyond = slice(edge, edge + extent)
    if len(margins) == 1:
        for plane in (0, 1):
            extended[plane, :edge, beyond] = margins[0][plane].astype(jnp.float32)
    else:
        take_step(extended, margins, own, edge // extent)
    visit_slots(lambda col: col + extent > edge, corners, counts, *held, extended, grad, work)
    margin_other[...] = grad[other, :edge, beyond].astype(jnp.bfloat16)
    margin_own[...] = grad[own, :edge, beyond].astype(jnp.bfloat16)
    for index, half in enumerate(halves):
        rows, cols = block_of(index // 4 * 2 + index % 2, extent)
        plane = (own, other)[index % 4 // 2]
        half[...] = grad[plane, rows, cols].astype(half.dtype)


WHOLE = pl.BlockSpec(memory_space=VMEM)
SCALAR = pl.BlockSpec(memory_space=SMEM)


def slot_cost(extent, slots):
    return pl.CostEstimate(
        flops=slots * 16 * extent**3, bytes_accessed=64 * extent * extent, transcendentals=0
    )


def load_step(corners, counts, tile, probe, patterns, table_set):
    extent = probe.shape[1]
    edge = tile.shape[1]
    loads = (probe, patterns, *table_set)
    image = jax.ShapeDtypeStruct((2, edge + SUBLANES, edge + extent), jnp.float32)
    extended, grad, *held = pl.pallas_call(
        functools.partial(load_kernel, edge),
        out_shape=[image, image] + [jax.ShapeDtypeStruct(v.shape, v.dtype) for v in loads],
        in_specs=[SCALAR] * 2 + [pl.BlockSpec(memory_space=HBM)] * 5,
        out_specs=[WHOLE] * 6,
        scratch_shapes=[pltpu.SemaphoreType.DMA((5,)), *work_space(extent, patterns.shape[0])],
        cost_estimate=slot_cost(extent, patterns.shape[0]),
        compiler_params=pltpu.CompilerParams(vmem_limit_bytes=LIMIT),
    )(corners, counts, *(pltpu.with_memory_space_constraint(v, HBM) for v in (tile, *loads)))
    return extended, grad, held


def inner_step(corners, counts, plane_index, held, extended, grad, edge, pieces):
    return pl.pallas_call(
        functools.partial(inner_kernel, edge),
        out_shape=[jax.ShapeDtypeStruct(v.shape, v.dtype) for v in (extended, grad)],
        in_specs=[SCALAR] * 3 + [WHOLE] * (6 + len(pieces)),
        out_specs=[WHOLE] * 2,
        scratch_shapes=work_space(held[0].shape[1], held[1].shape[0]),
        input_output_aliases={7: 0, 8: 1},
        cost_estimate=slot_cost(held[0].shape[1], held[1].shape[0]),
        compiler_params=pltpu.CompilerParams(vmem_limit_bytes=LIMIT),
    )(corners, counts, plane_index, *held, extended, grad, *pieces)


def outer_step(corners, counts, plane_index, held, extended, grad, edge, margins):
    extent = held[0].shape[1]
    half = jax.ShapeDtypeStruct((extent, extent), jnp.bfloat16)
    wide = jax.ShapeDtypeStruct((extent, extent), jnp.float32)
    outs = [jax.ShapeDtypeStruct(v.shape, v.dtype) for v in (extended, grad)]
    outs += [jax.ShapeDtypeStruct((edge, extent), jnp.bfloat16)] * 2
    outs += [wide] * 6 + [half] * 2
    extended, grad, margin_other, margin_own, *halves = pl.pallas_call(
        functools.partial(outer_kernel, edge),
        out_shape=outs,
        in_specs=[SCALAR] * 3 + [WHOLE] * (6 + len(margins)),
        out_specs=[WHOLE] * len(outs),
        scratch_shapes=work_space(held[0].shape[1], held[1].shape[0]),
        input_output_aliases={7: 0, 8: 1},
        cost_estimate=slot_cost(extent, held[1].shape[0]),
        compiler_params=pltpu.CompilerParams(vmem_limit_bytes=LIMIT),
    )(corners, counts, plane_index, *held, extended, grad, *margins)
    return extended, grad, (margin_other, margin_own), halves


def finish_kernel(block, plane_index, extended, own_top, own_low, other_top, other_low, *rest):
    out = rest[-1]
    own = plane_index[0]
    extent = own_top.shape[0]
    for plane, pieces in ((own, (own_top, own_low)), (1 - own, (other_top, other_low))):
        for half, piece in enumerate(pieces):
            rows, cols = block_of(2 * block + half, extent)
            step = LEARNING_RATE * piece[...].astype(jnp.float32)
            out[plane, rows] = extended[plane, rows, cols] - step


def finish(plane_index, extended, edge, pieces, block, partial):
    extent = pieces[0].shape[1]
    column = pl.BlockSpec((2, edge, extent), lambda step: (0, 0, block))
    earlier = [] if partial is None else [partial]
    return pl.pallas_call(
        functools.partial(finish_kernel, block),
        grid=(1,),
        out_shape=jax.ShapeDtypeStruct((2, edge, edge), jnp.float32),
        in_specs=[SCALAR] + [WHOLE] * 5 + [pl.BlockSpec(memory_space=pl.ANY)] * len(earlier),
        out_specs=column,
        input_output_aliases={6: 0} if earlier else {},
        cost_estimate=pl.CostEstimate(
            flops=4 * edge * edge, bytes_accessed=12 * edge * edge, transcendentals=0
        ),
        compiler_params=pltpu.CompilerParams(vmem_limit_bytes=LIMIT),
    )(plane_index, extended, *pieces, *earlier)


def tile_pairs(count, row_shift, col_shift, grid_rows):
    turn = TILE_COLS + TILE_COLS // 2
    pairs = []
    for source in range(count):
        cell = (source + turn) % count
        row = cell // TILE_COLS + row_shift
        col = cell % TILE_COLS + col_shift
        if 0 <= row < grid_rows and 0 <= col < TILE_COLS:
            pairs.append((source, (row * TILE_COLS + col - turn) % count))
    return pairs


def move(value, pairs, sharers, mask):
    both = [
        (source * sharers + pos, target * sharers + (pos ^ mask))
        for source, target in pairs
        for pos in range(sharers)
    ]
    return lax.ppermute(value, ("tile", "pos"), both)


def total_wide(*values):
    return sum(value.astype(jnp.float32) for value in values)


def total(*values):
    return total_wide(*values).astype(jnp.bfloat16)


def share(keep, send, here, sharers):
    got = [move(value, here, sharers, 1) for value in send]
    pair = [total(*values) for values in zip(keep, got)]
    far = [move(value, here, sharers, 3) for value in pair]
    own = [total(*values) for values in zip(pair, far)]
    other = [move(value, here, sharers, 1) for value in own]
    return own, other


def row_shards(object_tile, probe, patterns, corners, counts, table_set):
    tile_count = lax.axis_size("tile")
    sharers = lax.axis_size("pos")
    extent = probe.shape[1]
    here = [(tile, tile) for tile in range(tile_count)]
    onward = tile_pairs(tile_count, 0, 1, 1)
    back = tile_pairs(tile_count, 0, -1, 1)
    pos = lax.axis_index("pos")
    plane_index = ((pos ^ (pos // 2)) % 2).reshape(1).astype(jnp.int32)
    margin = move(object_tile[:, :, :extent].astype(jnp.bfloat16), back, sharers, 0)
    edge = object_tile.shape[1]
    extended, grad, held = load_step(corners, counts, object_tile, probe, patterns, table_set)
    margins = [margin]
    for repeat in range(ITERS):
        extended, grad, margin_send, halves = outer_step(
            corners, counts, plane_index, held, extended, grad, edge, margins
        )
        left_keep, left_send, right_keep, right_send = (halves[i : i + 2] for i in range(0, 8, 2))
        other_got, own_got = (move(value, onward, sharers, 0) for value in margin_send)
        right_own, right_other = share(right_keep, right_send, here, sharers)
        own_got, other_got = (
            [value[rows : rows + extent] for rows in (0, extent)] for value in (own_got, other_got)
        )
        left_keep = [total_wide(*pair) for pair in zip(left_keep, own_got)]
        left_send = [total(*pair) for pair in zip(left_send, other_got)]
        left_own, left_other = share(left_keep, left_send, here, sharers)
        if repeat < ITERS - 1:
            margins = [
                move(jnp.concatenate(value, 0), back, sharers, 0)
                for value in (left_own, left_other)
            ]
            pieces = (*left_own, *right_own, *left_other, *right_other)
            extended, grad = inner_step(
                corners, counts, plane_index, held, extended, grad, edge, pieces
            )
    refined = finish(plane_index, extended, edge, (*right_own, *right_other), 1, None)
    return finish(plane_index, extended, edge, (*left_own, *left_other), 0, refined)


def plain_kernel(corners, counts, extended, probe, patterns, first, second, out, *scratch):
    padded, grad, *work = scratch
    rows = extended.shape[1]
    padded[:, :rows, :] = extended[...]
    grad[...] = jnp.zeros_like(grad)
    every = lambda col_at: col_at >= 0
    visit_slots(every, corners, counts, probe, patterns, first, second, padded, grad, work)
    out[...] = grad[:, :rows, :]


def plain_step(corners, counts, extended, probe, patterns, table_set):
    extent = probe.shape[1]
    rows, cols = extended.shape[1:]
    whole = pl.BlockSpec(memory_space=VMEM)
    return pl.pallas_call(
        plain_kernel,
        out_shape=jax.ShapeDtypeStruct(extended.shape, jnp.float32),
        in_specs=[pl.BlockSpec(memory_space=SMEM)] * 2 + [whole] * 5,
        out_specs=whole,
        scratch_shapes=[
            pltpu.VMEM((2, rows + SUBLANES, cols), jnp.float32),
            pltpu.VMEM((2, rows + SUBLANES, cols), jnp.float32),
            *work_space(extent, patterns.shape[0]),
        ],
        compiler_params=pltpu.CompilerParams(vmem_limit_bytes=48 << 20),
    )(corners, counts, extended, probe, patterns, *table_set)


def grid_shards(object_tile, probe, patterns, corners, counts, table_set):
    tile_count = lax.axis_size("tile")
    sharers = lax.axis_size("pos")
    grid_rows = tile_count // TILE_COLS
    extent = probe.shape[1]
    edge = object_tile.shape[1]

    def shift(value, rows, cols):
        pairs = tile_pairs(tile_count, rows, cols, grid_rows)
        return move(value.astype(jnp.bfloat16), pairs, sharers, 0).astype(jnp.float32)

    for repeat in range(ITERS):
        upper = jnp.concatenate([object_tile, shift(object_tile[:, :, :extent], 0, -1)], 2)
        lower = jnp.concatenate(
            [
                shift(object_tile[:, :extent, :], -1, 0),
                shift(object_tile[:, :extent, :extent], -1, -1),
            ],
            2,
        )
        extended = jnp.concatenate([upper, lower], 1)
        grad = plain_step(corners, counts, extended, probe, patterns, table_set)
        interior = grad[:, :edge, :edge]
        interior = interior.at[:, :, :extent].add(shift(grad[:, :edge, edge:], 0, 1))
        interior = interior.at[:, :extent, :].add(shift(grad[:, edge:, :edge], 1, 0))
        interior = interior.at[:, :extent, :extent].add(shift(grad[:, edge:, edge:], 1, 1))
        object_tile = object_tile - LEARNING_RATE * lax.psum(
            interior.astype(jnp.bfloat16), "pos"
        ).astype(jnp.float32)
    return object_tile


def shards(object_tiles, probe, patterns, corners, counts):
    table_set = tables(probe.shape[1])
    one_row = lax.axis_size("tile") == TILE_COLS
    paired = lax.axis_size("pos") == 4 and object_tiles.shape[2] == 2 * probe.shape[1]
    run = row_shards if one_row and paired else grid_shards
    return run(object_tiles[0], probe, patterns, corners.T, counts, table_set)[None]


def solution(mesh):
    return jax.shard_map(
        shards,
        mesh=mesh,
        in_specs=(
            P("tile", None, None, None),
            P(),
            P(("tile", "pos"), None, None),
            P(("tile", "pos"), None),
            P(("tile", "pos")),
        ),
        out_specs=P("tile", None, None, None),
        check_vma=False,
    )
```
